32 devices in a mesh: batch: 1 (over z), head: 4 (over y), seq: 8 (over x, core).
Axes of the slice: x: 4, y: 4, z: 1, core: 2. Of those that a mesh axis runs over, the one named last changes fastest.
The devices are a block of a 4x4x8 slice.
Arguments:
- x_embed: bfloat16 [2048, 4096], P(('batch', 'seq'))
- positions: int32 [2048], P(('batch', 'seq'))
- w_q: bfloat16 [3, 4096, 32, 128], P(None, None, 'head')
- w_k: bfloat16 [3, 4096, 8, 128], P(None, None, 'head')
- w_v: bfloat16 [3, 4096, 8, 128], P(None, None, 'head')
- w_o: bfloat16 [3, 32, 128, 4096], P(None, 'head')
- w_gate: bfloat16 [3, 4096, 14336], P(None, None, 'head')
- w_up: bfloat16 [3, 4096, 14336], P(None, None, 'head')
- w_down: bfloat16 [3, 14336, 4096], P(None, 'head')
- norm_gain: bfloat16 [3, 4096], replicated
Outputs:
- output 1: bfloat16 [2048, 4096], P(('batch', 'seq'))
- output 2: bfloat16 [3, 2048, 8, 128], P(None, ('batch', 'seq'), 'head')
- output 3: bfloat16 [3, 2048, 8, 128], P(None, ('batch', 'seq'), 'head')
All inputs are finite; a program needn't handle non-finite values.
Results may differ from the reference program's by a relative error of at most 0.02.
Values are sent between devices in bfloat16 or wider.
A program may use at most 768 MiB of HBM per device.

```python
import math
import jax
import jax.numpy as jnp
from jax import lax

SEQ_LEN = 2048
D_MODEL = 4096
NUM_HEADS = 32
KV_HEADS = 8
HEAD_DIM = 128
FF_DIM = 14336
LAYERS = 3
QUERY_BLOCK = 128
ROPE_BASE = 500000
EPS = 1e-5


def draw_normal(rng_key, arr_shape, std_scale):
    return (jax.random.normal(rng_key, arr_shape, jnp.float32) * std_scale).astype(jnp.bfloat16)


def setup_inputs(seed: int = 0, part: int = 0) -> dict:
    shared_root, part_root = jax.random.split(jax.random.key(seed))
    part_key = jax.random.fold_in(part_root, part)
    key_embed, key_gap, key_offset = jax.random.split(part_key, 3)
    weight_keys = jax.random.split(shared_root, 8)
    logit_std = math.sqrt(0.5 * math.log(SEQ_LEN))
    qk_scale = math.sqrt(logit_std / D_MODEL)
    out_scale = 0.5 * SEQ_LEN ** 0.25 / math.sqrt(NUM_HEADS * HEAD_DIM)
    x_embed = draw_normal(key_embed, (SEQ_LEN, D_MODEL), 1.0)
    pos_gaps = jax.random.randint(key_gap, (SEQ_LEN,), 1, 4)
    offset = jax.random.randint(key_offset, (), 0, 1024)
    positions = (offset + jnp.cumsum(pos_gaps) - pos_gaps[0]).astype(jnp.int32)
    gains = 1.0 + 0.3 * jax.random.normal(weight_keys[7], (LAYERS, D_MODEL), jnp.float32)
    return {
        'x_embed': x_embed,
        'positions': positions,
        'w_q': draw_normal(weight_keys[0], (LAYERS, D_MODEL, NUM_HEADS, HEAD_DIM), qk_scale),
        'w_k': draw_normal(weight_keys[1], (LAYERS, D_MODEL, KV_HEADS, HEAD_DIM), qk_scale),
        'w_v': draw_normal(weight_keys[2], (LAYERS, D_MODEL, KV_HEADS, HEAD_DIM), D_MODEL ** -0.5),
        'w_o': draw_normal(weight_keys[3], (LAYERS, NUM_HEADS, HEAD_DIM, D_MODEL), out_scale),
        'w_gate': draw_normal(weight_keys[4], (LAYERS, D_MODEL, FF_DIM), D_MODEL ** -0.5),
        'w_up': draw_normal(weight_keys[5], (LAYERS, D_MODEL, FF_DIM), D_MODEL ** -0.5),
        'w_down': draw_normal(weight_keys[6], (LAYERS, FF_DIM, D_MODEL), 1.5 * FF_DIM ** -0.5),
        'norm_gain': gains.astype(jnp.bfloat16),
    }


def rms_norm(x_in, gain_row):
    x_f32 = x_in.astype(jnp.float32)
    inv_rms = lax.rsqrt(jnp.mean(x_f32 * x_f32, axis=-1, keepdims=True) + EPS)
    return (x_f32 * inv_rms * gain_row.astype(jnp.float32)).astype(jnp.bfloat16)


def rope_tables(positions):
    half_dim = HEAD_DIM // 2
    inv_freq = float(ROPE_BASE) ** (-(jnp.arange(half_dim, dtype=jnp.float32) * 2.0 / HEAD_DIM))
    angles = positions.astype(jnp.float32)[..., None] * inv_freq
    return jnp.cos(angles), jnp.sin(angles)


def apply_rope(heads_in, cos_t, sin_t):
    half_dim = heads_in.shape[-1] // 2
    heads_f32 = heads_in.astype(jnp.float32)
    first_half = heads_f32[..., :half_dim]
    second_half = heads_f32[..., half_dim:]
    cos_b = cos_t[..., None, :]
    sin_b = sin_t[..., None, :]
    rotated = jnp.concatenate([first_half * cos_b - second_half * sin_b, second_half * cos_b + first_half * sin_b], axis=-1)
    return rotated.astype(jnp.bfloat16)


def causal_attention(q_rot, k_rot, v_heads):
    group_size = NUM_HEADS // KV_HEADS
    logit_scale = 1.0 / math.sqrt(HEAD_DIM)
    num_blocks = SEQ_LEN // QUERY_BLOCK
    q_blocks = q_rot.reshape(num_blocks, QUERY_BLOCK, KV_HEADS, group_size, HEAD_DIM).astype(jnp.float32)
    k_f32 = k_rot.astype(jnp.float32)
    v_f32 = v_heads.astype(jnp.float32)
    key_index = jnp.arange(SEQ_LEN)

    def one_block(block_args):
        block_id, q_blk = block_args
        logits = jnp.einsum('qkgd,skd->qkgs', q_blk, k_f32) * logit_scale
        query_index = block_id * QUERY_BLOCK + jnp.arange(QUERY_BLOCK)
        allowed = (query_index[:, None] >= key_index[None, :])[:, None, None, :]
        logits = jnp.where(allowed, logits, -jnp.inf)
        row_max = jnp.max(logits, axis=-1, keepdims=True)
        prob_f32 = jnp.exp(logits - row_max)
        row_sum = jnp.sum(prob_f32, axis=-1, keepdims=True)
        prob_low = prob_f32.astype(jnp.bfloat16).astype(jnp.float32)
        return jnp.einsum('qkgs,skd->qkgd', prob_low, v_f32) / row_sum

    block_out = lax.map(one_block, (jnp.arange(num_blocks), q_blocks))
    return block_out.reshape(SEQ_LEN, NUM_HEADS * HEAD_DIM).astype(jnp.bfloat16)


def reference(x_embed, positions, w_q, w_k, w_v, w_o, w_gate, w_up, w_down, norm_gain):
    cos_t, sin_t = rope_tables(positions)

    def layer_step(x_cur, layer_weights):
        wq_l, wk_l, wv_l, wo_l, wg_l, wu_l, wd_l, gain_row = layer_weights
        normed = rms_norm(x_cur, gain_row)
        q_proj = jnp.dot(normed, wq_l.reshape(D_MODEL, NUM_HEADS * HEAD_DIM), preferred_element_type=jnp.float32).astype(jnp.bfloat16)
        k_proj = jnp.dot(normed, wk_l.reshape(D_MODEL, KV_HEADS * HEAD_DIM), preferred_element_type=jnp.float32).astype(jnp.bfloat16)
        v_proj = jnp.dot(normed, wv_l.reshape(D_MODEL, KV_HEADS * HEAD_DIM), preferred_element_type=jnp.float32).astype(jnp.bfloat16)
        q_rot = apply_rope(q_proj.reshape(SEQ_LEN, NUM_HEADS, HEAD_DIM), cos_t, sin_t)
        k_rot = apply_rope(k_proj.reshape(SEQ_LEN, KV_HEADS, HEAD_DIM), cos_t, sin_t)
        v_heads = v_proj.reshape(SEQ_LEN, KV_HEADS, HEAD_DIM)
        attn_heads = causal_attention(q_rot, k_rot, v_heads)
        attn_part = jnp.dot(attn_heads, wo_l.reshape(NUM_HEADS * HEAD_DIM, D_MODEL), preferred_element_type=jnp.float32)
        gate_f32 = jnp.dot(normed, wg_l, preferred_element_type=jnp.float32)
        up_f32 = jnp.dot(normed, wu_l, preferred_element_type=jnp.float32)
        hidden = (jax.nn.silu(gate_f32) * up_f32).astype(jnp.bfloat16)
        mlp_part = jnp.dot(hidden, wd_l, preferred_element_type=jnp.float32)
        update = (attn_part + mlp_part).astype(jnp.bfloat16)
        x_next = (x_cur.astype(jnp.float32) + update.astype(jnp.float32)).astype(jnp.bfloat16)
        return x_next, (k_rot, v_heads)

    stacked = (w_q, w_k, w_v, w_o, w_gate, w_up, w_down, norm_gain)
    x_out, caches = lax.scan(layer_step, x_embed, stacked)
    return x_out, caches[0], caches[1]
```

```python
import functools
import math
import jax
import jax.numpy as jnp
from jax import lax
from jax.experimental import pallas as pl
from jax.experimental.pallas import tpu as pltpu
from jax.sharding import PartitionSpec as P

ROPE_BASE = 500000.0
EPS = 1e-5
F32 = jnp.float32
BF16 = jnp.bfloat16
MESH = pl.DeviceIdType.MESH

NSTREAM = 4
NGUBUF = 3
NWDBUF = 3


def rope_tables(positions, head_dim):
    half_dim = head_dim // 2
    inv_freq = ROPE_BASE ** (-(jnp.arange(half_dim, dtype=F32) * 2.0 / head_dim))
    angles = positions.astype(F32)[..., None] * inv_freq
    cos_t, sin_t = jnp.cos(angles), jnp.sin(angles)
    return jnp.stack([jnp.concatenate([cos_t, cos_t], -1), jnp.concatenate([-sin_t, sin_t], -1)])


def decoder_kernel(dims, x_h, cs_h, wqkv_h, wo_h, wg_h, wu_h, wd_h, gain_v, xout_h, kvout_h,
                   X, H, QKVS, Q, ATT, HID, G, PS, PAIR, RS, TAB, KV, GU, WD, WO, WQKV, MX, LS, ACC,
                   s_xin, s_xs, s_xr, s_tab, s_gu, s_wd, s_wo, s_wqkv, s_ps, s_pr, s_rss, s_rsr, s_ags, s_agr,
                   s_fws, s_fwr, s_kvs, s_kvr, s_cl, s_cs, s_cr, s_out):
    L, T, D, NY, NX, GH, HD, FF, FT, BW = (dims[k] for k in ('L', 'T', 'D', 'NY', 'NX', 'GH', 'HD', 'FF', 'FT', 'BW'))
    NB = 2 * NY
    NGU = FF // FT
    QW = GH * HD
    NQ = (QW + 2 * HD) // (2 * HD)
    NS = NSTREAM
    R = T // NS
    NE = (2 * NY - 1) * NS
    scale = 1.0 / math.sqrt(HD)

    y = lax.axis_index('head')
    s = lax.axis_index('seq')
    c = lax.rem(s, 2)
    xx = lax.div(s, 2)
    partner = {'seq': s + 1 - 2 * c}
    own0 = c * NY
    oth0 = (1 - c) * NY

    def rcopy(src, dst, ss, rs, dev):
        return pltpu.make_async_remote_copy(src_ref=src, dst_ref=dst, send_sem=ss, recv_sem=rs, device_id=dev, device_id_type=MESH)

    def lcopy(src, dst, sem):
        return pltpu.make_async_copy(src, dst, sem)

    def gu_copies(i):
        slot = lax.rem(i, NGUBUF)
        hs = lax.div(i, NGU)
        n = lax.rem(i, NGU)
        l = lax.div(hs, 2)
        cols = pl.ds(pl.multiple_of(c * FF + n * FT, FT), FT)
        return (lcopy(wg_h.at[l, :, cols], GU.at[slot, 0], s_gu.at[slot, 0]),
                lcopy(wu_h.at[l, :, cols], GU.at[slot, 1], s_gu.at[slot, 1]))

    def block_of(n):
        return jnp.where(n < NY, oth0 + n, own0 + lax.rem(y + 1 + n, NY))

    def wd_copy(i):
        slot = lax.rem(i, NWDBUF)
        hs = lax.div(i, NB)
        n = lax.rem(i, NB)
        l = lax.div(hs, 2)
        rows = pl.ds(pl.multiple_of(c * FF, FT), FF)
        cols = pl.ds(pl.multiple_of(block_of(n) * BW, BW), BW)
        return lcopy(wd_h.at[l, rows, cols], WD.at[slot], s_wd.at[slot])

    def wo_copy(l):
        return lcopy(wo_h.at[l, pl.ds(pl.multiple_of(c * QW, QW), QW), :], WO, s_wo.at[0])

    def wqkv_copy(l):
        return lcopy(wqkv_h.at[l], WQKV, s_wqkv.at[0])

    wqkv_copy(0).start()
    for i in range(NGUBUF):
        for cp in gu_copies(i):
            cp.start()
    for i in range(NWDBUF):
        wd_copy(i).start()
    wo_copy(0).start()

    barrier = pltpu.get_barrier_semaphore()
    peers = [partner, {'head': lax.rem(y + 1, NY)}, {'head': lax.rem(y + NY - 1, NY)}]
    peers += [{'seq': lax.rem(s + 2 * d, 2 * NX)} for d in range(1, NX)]
    for peer in peers:
        pl.semaphore_signal(barrier, inc=1, device_id=peer, device_id_type=MESH)
    pl.semaphore_wait(barrier, len(peers))

    def xin_local(b):
        return lcopy(x_h.at[:, pl.ds(b * BW, BW)], X.at[c, b], s_xin.at[b])

    def xin_remote(b):
        return rcopy(x_h.at[:, pl.ds(b * BW, BW)], X.at[c, b], s_xs.at[b], s_xr.at[b], partner)

    def tab_local():
        return lcopy(cs_h, TAB.at[c], s_tab.at[0])

    def tab_remote():
        return rcopy(cs_h, TAB.at[c], s_tab.at[1], s_tab.at[2], partner)

    for b in range(NB):
        xin_remote(b).start()
        xin_local(b).start()
    tab_remote().start()
    tab_local().start()
    for b in range(NB):
        xin_local(b).wait()
        xin_remote(b).wait()
    tab_local().wait()
    tab_remote().wait()

    def rows_of(st):
        return pl.ds(pl.multiple_of(st * R, R), R)

    def sign_of(st):
        return 1 - 2 * lax.rem(st, 2)

    def ring_dev(st):
        return {'head': lax.rem(y + sign_of(st) + NY, NY)}

    def blk_at(st, k):
        return lax.rem(y - sign_of(st) * k + 2 * NY, NY)

    def pair_copy(j, bb):
        return rcopy(PS.at[j, oth0 + bb], PAIR.at[j, bb], s_ps.at[j, bb], s_pr.at[j, bb], partner)

    def rs_copy(j, t, st):
        return rcopy(PS.at[j, own0 + blk_at(st, 1 + t), rows_of(st)], RS.at[j, t, rows_of(st)],
                     s_rss.at[j, t, st], s_rsr.at[j, t, st], ring_dev(st))

    def ag_copy(j, t, st):
        ref = X.at[j, own0 + blk_at(st, t), rows_of(st)]
        return rcopy(ref, ref, s_ags.at[j, t, st], s_agr.at[j, t, st], ring_dev(st))

    def fw_copy(j, t, st):
        ref = X.at[j, own0 + blk_at(st, t), rows_of(st)]
        return rcopy(ref, ref, s_fws.at[j, t, st], s_fwr.at[j, t, st], partner)

    def service(j, e):
        kind = lax.div(e, NS)
        st = lax.rem(e, NS)
        rows = rows_of(st)

        @pl.when(e == 0)
        def _():
            for bb in range(NY):
                pair_copy(j, bb).wait_recv()

        @pl.when(kind == 0)
        def _():
            bb = blk_at(st, 1)
            PS[j, own0 + bb, rows] += PAIR[j, bb, rows]
            rs_copy(j, 0, st).start()

        @pl.when((kind >= 1) & (kind < NY - 1))
        def _():
            t = kind - 1
            rs_copy(j, t, st).wait_recv()
            bb = blk_at(st, t + 2)
            PS[j, own0 + bb, rows] = PS[j, own0 + bb, rows] + PAIR[j, bb, rows] + RS[j, t, rows]
            rs_copy(j, t + 1, st).start()

        @pl.when(kind == NY - 1)
        def _():
            rs_copy(j, NY - 2, st).wait_recv()
            total = PS[j, own0 + y, rows] + PAIR[j, y, rows] + RS[j, NY - 2, rows]
            upd = total.astype(BF16).astype(F32)
            X[j, own0 + y, rows] = (X[j, own0 + y, rows].astype(F32) + upd).astype(BF16)
            ag_copy(j, 0, st).start()
            fw_copy(j, 0, st).start()

        @pl.when((kind >= NY) & (kind < 2 * NY - 1))
        def _():
            t = kind - NY
            ag_copy(j, t, st).wait_recv()

            @pl.when(t < NY - 2)
            def _():
                ag_copy(j, t + 1, st).start()
            fw_copy(j, t + 1, st).start()

    def drain(j, e0):
        def body(e, carry):
            service(j, e)
            return carry
        lax.fori_loop(e0, NE, body, 0)
        for bb in range(NY):
            pair_copy(j, bb).wait_send()

        def ends(st, carry):
            for t in range(NY):
                fw_copy(j, t, st).wait_recv()
            for t in range(NY - 1):
                rs_copy(j, t, st).wait_send()
                ag_copy(j, t, st).wait_send()
            for t in range(NY):
                fw_copy(j, t, st).wait_send()
            return carry
        lax.fori_loop(0, NS, ends, 0)

    def norm(j, l, slot):
        RG = T // 4

        def body(r, carry):
            rows = pl.ds(pl.multiple_of(r * RG, RG), RG)
            ssq = jnp.zeros((RG, BW), F32)
            for b in range(NB):
                xb = X[j, b, rows, :].astype(F32)
                ssq = ssq + xb * xb
            inv = lax.rsqrt(jnp.sum(ssq, axis=-1, keepdims=True) * (1.0 / D) + EPS)
            for b in range(NB):
                xb = X[j, b, rows, :].astype(F32)
                H[rows, b * BW:(b + 1) * BW] = (xb * inv * gain_v[l, :, b * BW:(b + 1) * BW]).astype(BF16)
            slot(r)
            return carry
        lax.fori_loop(0, 4, body, 0)

    def push_copy(j, l, d):
        g = 2 * xx + j
        return rcopy(KV.at[l, g], KV.at[l, g], s_kvs.at[j, d - 1], s_kvr.at[l * (2 * NX) + g], {'seq': lax.rem(s + 2 * d, 2 * NX)})

    def recv_wait(l, g):
        rcopy(KV.at[l, g], KV.at[l, g], s_kvs.at[0, 0], s_kvr.at[l * (2 * NX) + g], partner).wait_recv()

    def cache_local(l, j):
        return lcopy(KV.at[l, 2 * xx + j], kvout_h.at[l, c], s_cl.at[l])

    def cache_remote(l, j):
        return rcopy(KV.at[l, 2 * xx + j], kvout_h.at[l, c], s_cs.at[l], s_cr.at[l], partner)

    def qkv(j, l, slot):
        def body(n, carry):
            cols = pl.ds(pl.multiple_of(n * 2 * HD, 2 * HD), 2 * HD)
            QKVS[n] = jnp.dot(H[...], WQKV[:, cols], preferred_element_type=F32).astype(BF16)
            slot(n)
            return carry
        lax.fori_loop(0, NQ, body, 0)
        g = 2 * xx + j

        def rot(val):
            vf = val.astype(F32)
            return (vf * TAB[j, 0] + pltpu.roll(vf, HD // 2, 1) * TAB[j, 1]).astype(BF16)
        KV[l, g, 0] = rot(QKVS[NQ - 1, :, 0:HD])
        KV[l, g, 1] = QKVS[NQ - 1, :, HD:2 * HD]
        for d in range(1, NX):
            @pl.when(xx + d < NX)
            def _():
                push_copy(j, l, d).start()

        @pl.when(c == j)
        def _():
            cache_local(l, j).start()

        @pl.when(c != j)
        def _():
            cache_remote(l, j).start()
        for h in range(GH):
            Q[j, h] = rot(QKVS[h // 2, :, (h % 2) * HD:(h % 2 + 1) * HD])

    def push_done(j, l):
        for d in range(1, NX):
            @pl.when(xx + d < NX)
            def _():
                push_copy(j, l, d).wait_send()

    def attention(j, l, slot):
        g = 2 * xx + j
        nt = (((1,), (1,)), ((), ()))

        row_i = lax.broadcasted_iota(jnp.int32, (T, T), 0)
        col_i = lax.broadcasted_iota(jnp.int32, (T, T), 1)
        for h in range(GH):
            sc = lax.dot_general(Q[j, h], KV[l, g, 0], nt, preferred_element_type=F32) * scale
            sc = jnp.where(row_i >= col_i, sc, -jnp.inf)
            m = jnp.max(sc, axis=1, keepdims=True)
            p = jnp.exp(sc - m)
            MX[h] = jnp.broadcast_to(m, (T, HD))
            LS[h] = jnp.broadcast_to(jnp.sum(p, axis=1, keepdims=True), (T, HD))
            ACC[h] = jnp.dot(p.astype(BF16), KV[l, g, 1], preferred_element_type=F32)
        slot(0)

        def body(i, carry):
            if j == 0:
                gi = jnp.where(i < xx, 2 * i, 2 * (i - xx) + 1)
                recv_wait(l, gi)
            else:
                gi = i
            for h in range(GH):
                sc = lax.dot_general(Q[j, h], KV[l, gi, 0], nt, preferred_element_type=F32) * scale
                m_old = MX[h]
                m_new = jnp.maximum(m_old, jnp.max(sc, axis=1, keepdims=True))
                p = jnp.exp(sc - jnp.concatenate([m_new] * (T // HD), axis=1))
                alpha = jnp.exp(m_old - m_new)
                MX[h] = m_new
                LS[h] = LS[h] * alpha + jnp.sum(p, axis=1, keepdims=True)
                ACC[h] = ACC[h] * alpha + jnp.dot(p.astype(BF16), KV[l, gi, 1], preferred_element_type=F32)
            slot(i + 1)
            return carry
        lax.fori_loop(0, 2 * xx + j, body, 0)
        for h in range(GH):
            ATT[:, h * HD:(h + 1) * HD] = (ACC[h] / LS[h]).astype(BF16)

    def gate_up(j, l, slot):
        def body(n, carry):
            i = (2 * l + j) * NGU + n
            sl = lax.rem(i, NGUBUF)
            cg, cu = gu_copies(i)
            cg.wait()
            G[...] = jnp.dot(H[...], GU[sl, 0], preferred_element_type=F32)
            slot(2 * n)
            cu.wait()
            up = jnp.dot(H[...], GU[sl, 1], preferred_element_type=F32)
            gate = G[...]
            HID[:, pl.ds(pl.multiple_of(n * FT, FT), FT)] = (gate * jax.nn.sigmoid(gate) * up).astype(BF16)

            @pl.when(i + NGUBUF < 2 * L * NGU)
            def _():
                for cp in gu_copies(i + NGUBUF):
                    cp.start()
            slot(2 * n + 1)
            return carry
        lax.fori_loop(0, NGU, body, 0)

    def o_tile(blk):
        cols = pl.ds(pl.multiple_of(blk * BW, BW), BW)
        return jnp.dot(ATT[...], WO[:, cols], preferred_element_type=F32)

    def send_pair(j, n):
        @pl.when(n < NY)
        def _():
            pair_copy(j, n).start()

    def down(j, l, with_o, slot):
        def body(n, carry):
            i = (2 * l + j) * NB + n
            sl = lax.rem(i, NWDBUF)
            blk = block_of(n)
            wd_copy(i).wait()
            val = jnp.dot(HID[...], WD[sl], preferred_element_type=F32)
            if with_o:
                val = val + o_tile(blk)
            PS[j, blk] = val

            @pl.when(i + NWDBUF < 2 * L * NB)
            def _():
                wd_copy(i + NWDBUF).start()
            if with_o:
                send_pair(j, n)
            slot(n)
            return carry
        lax.fori_loop(0, NB, body, 0)

    def o_proj(j, l):
        def body(n, carry):
            blk = block_of(n)
            PS[j, blk] += o_tile(blk)
            send_pair(j, n)
            return carry
        lax.fori_loop(0, NB, body, 0)

    def layer(l, carry):
        def sv1(e):
            @pl.when((l > 0) & (e < NE))
            def _():
                service(1, e)

        def sv0(e):
            @pl.when(e < NE)
            def _():
                service(0, e)

        norm(0, l, lambda k: sv1(k))
        wqkv_copy(l).wait()
        qkv(0, l, lambda k: sv1(4 + k))
        e1 = 4 + NQ
        gate_up(0, l, lambda k: sv1(e1 + k))
        down(0, l, False, lambda k: sv1(e1 + 2 * NGU + k))

        @pl.when(l > 0)
        def _():
            drain(1, e1 + 2 * NGU + NB)

        norm(1, l, lambda k: None)
        qkv(1, l, lambda k: None)

        @pl.when(l + 1 < L)
        def _():
            wqkv_copy(l + 1).start()
        attention(0, l, lambda k: None)
        wo_copy(l).wait()
        o_proj(0, l)

        gate_up(1, l, lambda k: sv0(k))
        e0 = 2 * NGU
        attention(1, l, lambda k: sv0(e0 + k))
        e0 = e0 + 2 * xx + 2
        down(1, l, True, lambda k: sv0(e0 + k))

        @pl.when(l + 1 < L)
        def _():
            wo_copy(l + 1).start()
        drain(0, e0 + NB)
        push_done(0, l)
        push_done(1, l)
        return carry

    lax.fori_loop(0, L, layer, 0)
    drain(1, 0)

    for b in range(NB):
        lcopy(X.at[c, b], xout_h.at[:, pl.ds(b * BW, BW)], s_out.at[b]).start()
    for b in range(NB):
        lcopy(X.at[c, b], xout_h.at[:, pl.ds(b * BW, BW)], s_out.at[b]).wait()
    for l in range(L):
        cache_local(l, 0).wait()
        cache_remote(l, 0).wait()


def solution(mesh):
    NY = mesh.shape['head']
    NX = mesh.shape['seq'] // 2
    row_spec = P(('batch', 'seq'), None)
    pos_spec = P(('batch', 'seq'))
    head_spec = P(None, None, 'head', None)
    out_proj_spec = P(None, 'head', None, None)
    col_spec = P(None, None, 'head')
    down_spec = P(None, 'head', None)
    cache_spec = P(None, ('batch', 'seq'), 'head', None)

    def local_forward(x_loc, pos_loc, w_q, w_k, w_v, w_o, w_gate, w_up, w_down, norm_gain):
        T, D = x_loc.shape
        L, _, q_local, HD = w_q.shape
        GH = q_local // 2
        FF = w_gate.shape[2] // 2
        BW = D // (2 * NY)
        FT = 256 if FF % 256 == 0 else 128
        dims = dict(L=L, T=T, D=D, NY=NY, NX=NX, GH=GH, HD=HD, FF=FF, FT=FT, BW=BW)
        core = lax.rem(lax.axis_index('seq'), 2)
        wq_c = lax.dynamic_slice_in_dim(w_q, core * GH, GH, 2).reshape(L, D, GH * HD)
        wk_c = lax.dynamic_slice_in_dim(w_k, core, 1, 2).reshape(L, D, HD)
        wv_c = lax.dynamic_slice_in_dim(w_v, core, 1, 2).reshape(L, D, HD)
        wqkv = jnp.concatenate([wq_c, wk_c, wv_c], axis=2)
        wo = w_o.reshape(L, q_local * HD, D)
        gain = norm_gain.astype(F32).reshape(L, 1, D)
        tab = rope_tables(pos_loc, HD)
        QW = GH * HD
        NB = 2 * NY
        NQ = (QW + 2 * HD) // (2 * HD)
        any_spec = pl.BlockSpec(memory_space=pl.ANY)
        dma = pltpu.SemaphoreType.DMA
        V = pltpu.VMEM
        scratch = [
            V((2, NB, T, BW), BF16), V((T, D), BF16), V((NQ, T, 2 * HD), BF16), V((2, GH, T, HD), BF16), V((T, QW), BF16),
            V((T, FF), BF16), V((T, FT), F32), V((2, NB, T, BW), F32), V((2, NY, T, BW), F32), V((2, NY - 1, T, BW), F32),
            V((2, 2, T, HD), F32), V((L, 2 * NX, 2, T, HD), BF16), V((NGUBUF, 2, D, FT), BF16), V((NWDBUF, FF, BW), BF16),
            V((QW, D), BF16), V((D, QW + 2 * HD), BF16), V((GH, T, HD), F32), V((GH, T, HD), F32), V((GH, T, HD), F32),
            dma((NB,)), dma((NB,)), dma((NB,)), dma((3,)), dma((NGUBUF, 2)), dma((NWDBUF,)), dma((1,)), dma((1,)),
            dma((2, NY)), dma((2, NY)), dma((2, NY - 1, NSTREAM)), dma((2, NY - 1, NSTREAM)),
            dma((2, NY - 1, NSTREAM)), dma((2, NY - 1, NSTREAM)), dma((2, NY, NSTREAM)), dma((2, NY, NSTREAM)),
            dma((2, NX)), dma((L * 2 * NX,)), dma((L,)), dma((L,)), dma((L,)), dma((NB,)),
        ]
        x_out, kv = pl.pallas_call(
            functools.partial(decoder_kernel, dims),
            out_shape=(jax.ShapeDtypeStruct((T, D), BF16), jax.ShapeDtypeStruct((L, 2, 2, T, HD), BF16)),
            in_specs=[any_spec] * 7 + [pl.BlockSpec(memory_space=pltpu.VMEM)],
            out_specs=(any_spec, any_spec),
            scratch_shapes=scratch,
            compiler_params=pltpu.CompilerParams(collective_id=0, has_side_effects=True, vmem_limit_bytes=67043328),
            name='decoder',
        )(x_loc, tab, wqkv, wo, w_gate, w_up, w_down, gain)
        kv = jnp.transpose(kv, (2, 0, 3, 1, 4))
        return x_out, kv[0], kv[1]

    return jax.shard_map(local_forward, mesh=mesh, in_specs=(row_spec, pos_spec, head_spec, head_spec, head_spec, out_proj_spec, col_spec, col_spec, down_spec, P(None, None)), out_specs=(row_spec, cache_spec, cache_spec), check_vma=False)
```

```python
import functools
import math
import jax
import jax.numpy as jnp
from jax import lax
from jax.experimental import pallas as pl
from jax.experimental.pallas import tpu as pltpu
from jax.sharding import PartitionSpec as P

ROPE_BASE = 500000.0
EPS = 1e-5
F32 = jnp.float32
BF16 = jnp.bfloat16
MESH = pl.DeviceIdType.MESH

NSTREAM = 4
NGUBUF = 3
NWDBUF = 4
RATE = ((1, 1), (4, 3))
NAHEAD = 2
NRAW = 4


def rope_tables(positions, head_dim):
    half_dim = head_dim // 2
    inv_freq = ROPE_BASE ** (-(jnp.arange(half_dim, dtype=F32) * 2.0 / head_dim))
    angles = positions.astype(F32)[..., None] * inv_freq
    cos_t, sin_t = jnp.cos(angles), jnp.sin(angles)
    return jnp.stack([jnp.concatenate([cos_t, cos_t], -1), jnp.concatenate([-sin_t, sin_t], -1)])


def decoder_kernel(dims, x_h, cs_h, wq_h, wk_h, wv_h, wo_h, wg_h, wu_h, wd_h, gain_v, xout_h, kvout_h,
                   X, H, QKVS, Q, ATT, HID, G, PS, PAIR, RS, TAB, KV, GU, WD, WO, WQKV, MX, LS, ACC, RAW, WIDE,
                   s_xin, s_xs, s_xr, s_tab, s_gu, s_wd, s_wo, s_raw, s_ps, s_pr, s_rss, s_rsr, s_ags, s_agr,
                   s_fws, s_fwr, s_kvs, s_kvr, s_cl, s_cs, s_cr, s_out):
    L, T, D, NY, NX, GH, HD, FF, FT, BW = (dims[k] for k in ('L', 'T', 'D', 'NY', 'NX', 'GH', 'HD', 'FF', 'FT', 'BW'))
    NB = 2 * NY
    NGU = FF // FT
    QW = GH * HD
    NQ = (QW + 2 * HD) // (2 * HD)
    NS = NSTREAM
    R = T // NS
    NE = 5 * NS
    scale = 1.0 / math.sqrt(HD)

    y = lax.axis_index('head')
    s = lax.axis_index('seq')
    c = lax.rem(s, 2)
    xx = lax.div(s, 2)
    partner = {'seq': s + 1 - 2 * c}
    own0 = c * NY
    oth0 = (1 - c) * NY

    def rcopy(src, dst, ss, rs, dev):
        return pltpu.make_async_remote_copy(src_ref=src, dst_ref=dst, send_sem=ss, recv_sem=rs, device_id=dev, device_id_type=MESH)

    def lcopy(src, dst, sem):
        return pltpu.make_async_copy(src, dst, sem)

    def gu_copies(i):
        slot = lax.rem(i, NGUBUF)
        hs = lax.div(i, NGU)
        n = lax.rem(i, NGU)
        l = lax.div(hs, 2)
        cols = pl.ds(pl.multiple_of(c * FF + n * FT, FT), FT)
        return (lcopy(wg_h.at[l, :, cols], GU.at[slot, 0], s_gu.at[slot, 0]),
                lcopy(wu_h.at[l, :, cols], GU.at[slot, 1], s_gu.at[slot, 1]))

    assert NY == 4
    ya = y + 1 - 2 * lax.rem(y, 2)
    yb = NY - 1 - y
    y2 = lax.rem(y + 2, NY)

    def ring_block(n):
        return jnp.where(n == 0, y2, jnp.where(n == 1, ya, jnp.where(n == 2, yb, y)))

    def block_of(n):
        return jnp.where(n < NY, oth0, own0) + ring_block(lax.rem(n, NY))

    def wd_copy(i):
        slot = lax.rem(i, NWDBUF)
        hs = lax.div(i, NB)
        n = lax.rem(i, NB)
        l = lax.div(hs, 2)
        rows = pl.ds(pl.multiple_of(c * FF, FT), FF)
        cols = pl.ds(pl.multiple_of(block_of(n) * BW, BW), BW)
        return lcopy(wd_h.at[l, rows, cols], WD.at[slot], s_wd.at[slot])

    def wo_copy(l):
        return lcopy(wo_h.at[l, pl.ds(pl.multiple_of(c * QW, QW), QW), :], WO, s_wo.at[0])

    RP = RAW.shape[1]
    QROWS, KROWS = 2 * GH, 2
    NPQ, NPK = D * QROWS // RP, D * KROWS // RP

    def raw_copy(l, kind, n):
        ref, base = ((wq_h, 0), (wk_h, NPQ), (wv_h, NPQ + NPK))[kind]
        slot = lax.rem(base + n, NRAW)
        return lcopy(ref.at[l, pl.ds(pl.multiple_of(n * RP, RP), RP), :], RAW.at[slot], s_raw.at[slot])

    def raw_start(l, p):
        for kind, lo, hi in ((0, 0, NPQ), (1, NPQ, NPQ + NPK), (2, NPQ + NPK, NPQ + 2 * NPK)):
            @pl.when((p >= lo) & (p < hi))
            def _():
                raw_copy(l, kind, p - lo).start()

    def build_qkv(l, slot):
        for kind, lo, count in ((0, 0, NPQ), (1, NPQ, NPK), (2, NPQ + NPK, NPK)):
            heads, step = (GH, QROWS) if kind == 0 else (1, KROWS)
            kk = RP // step

            def body(n, carry):
                p = lo + n
                raw_copy(l, kind, n).wait()
                WIDE[...] = RAW[lax.rem(p, NRAW)].astype(F32)
                raw_start(l, p + NRAW)
                for h in range(heads):
                    col = h * HD if kind == 0 else QW + (kind - 1) * HD
                    WQKV[pl.ds(pl.multiple_of(n * kk, kk), kk), col:col + HD] = WIDE[pl.ds(c * heads + h, kk, stride=step), :].astype(BF16)
                slot(p)
                return carry
            lax.fori_loop(0, count, body, 0)

    for p in range(NRAW):
        raw_start(0, jnp.int32(p))

    barrier = pltpu.get_barrier_semaphore()
    peers = [partner, {'head': ya}, {'head': yb}]
    peers += [{'seq': lax.rem(s + 2 * d, 2 * NX)} for d in range(1, NX)]
    for peer in peers:
        pl.semaphore_signal(barrier, inc=1, device_id=peer, device_id_type=MESH)
    pl.semaphore_wait(barrier, len(peers))

    def xin_local(b):
        return lcopy(x_h.at[:, pl.ds(b * BW, BW)], X.at[c, b], s_xin.at[b])

    def xin_remote(b):
        return rcopy(x_h.at[:, pl.ds(b * BW, BW)], X.at[c, b], s_xs.at[b], s_xr.at[b], partner)

    def tab_local():
        return lcopy(cs_h, TAB.at[c], s_tab.at[0])

    def tab_remote():
        return rcopy(cs_h, TAB.at[c], s_tab.at[1], s_tab.at[2], partner)

    for b in range(NB):
        xin_remote(b).start()
        xin_local(b).start()
    tab_remote().start()
    tab_local().start()
    build_qkv(0, lambda k: None)
    for i in range(NGUBUF):
        for cp in gu_copies(jnp.int32(i)):
            cp.start()
    for i in range(NWDBUF):
        wd_copy(jnp.int32(i)).start()
    wo_copy(0).start()
    for b in range(NB):
        xin_local(b).wait()
        xin_remote(b).wait()
    tab_local().wait()
    tab_remote().wait()

    def rows_of(st):
        return pl.ds(pl.multiple_of(st * R, R), R)

    def side(st, first):
        return jnp.where(lax.rem(st, 2) == (0 if first else 1), ya, yb)

    def pair_copy(j, bb):
        return rcopy(PS.at[j, oth0 + bb], PAIR.at[j, bb], s_ps.at[j, bb], s_pr.at[j, bb], partner)

    def rs_copy(j, t, st):
        dev = side(st, t < 2)
        src = y2 if t == 1 else dev
        return rcopy(PS.at[j, own0 + src, rows_of(st)], RS.at[j, t, rows_of(st)],
                     s_rss.at[j, t, st], s_rsr.at[j, t, st], {'head': dev})

    def ag_copy(j, t, st):
        src = side(st, False) if t == 2 else y
        ref = X.at[j, own0 + src, rows_of(st)]
        return rcopy(ref, ref, s_ags.at[j, t, st], s_agr.at[j, t, st], {'head': side(st, t > 0)})

    def fw_copy(j, t, st):
        src = (y, side(st, False), side(st, True), y2)[t]
        ref = X.at[j, own0 + src, rows_of(st)]
        return rcopy(ref, ref, s_fws.at[j, t, st], s_fwr.at[j, t, st], partner)

    def service(j, e):
        kind = lax.div(e, NS)
        st = lax.rem(e, NS)
        rows = rows_of(st)

        @pl.when(kind < 3)
        def _():
            @pl.when(kind == 0)
            def _():
                @pl.when(st == 0)
                def _():
                    pair_copy(j, y2).wait_recv()
                    pair_copy(j, ya).wait_recv()

                @pl.when(st == 1)
                def _():
                    pair_copy(j, yb).wait_recv()
                PS[j, own0 + y2, rows] += PAIR[j, y2, rows]
                rs_copy(j, 1, st).start()
                blk = side(st, True)
                PS[j, own0 + blk, rows] += PAIR[j, blk, rows]
                rs_copy(j, 0, st).start()

            @pl.when(kind == 1)
            def _():
                rs_copy(j, 1, st).wait_recv()
                blk = side(st, False)
                PS[j, own0 + blk, rows] = PS[j, own0 + blk, rows] + PAIR[j, blk, rows] + RS[j, 1, rows]
                rs_copy(j, 2, st).start()

            @pl.when(kind == 2)
            def _():
                @pl.when(st == 0)
                def _():
                    pair_copy(j, y).wait_recv()
                rs_copy(j, 0, st).wait_recv()
                rs_copy(j, 2, st).wait_recv()
                total = (PS[j, own0 + y, rows] + PAIR[j, y, rows]) + (RS[j, 0, rows] + RS[j, 2, rows])
                upd = total.astype(BF16).astype(F32)
                X[j, own0 + y, rows] = (X[j, own0 + y, rows].astype(F32) + upd).astype(BF16)
                ag_copy(j, 0, st).start()
                ag_copy(j, 1, st).start()
                fw_copy(j, 0, st).start()

        @pl.when(kind >= 3)
        def _():
            @pl.when(kind == 3)
            def _():
                ag_copy(j, 0, st).wait_recv()
                ag_copy(j, 2, st).start()
                fw_copy(j, 1, st).start()

            @pl.when(kind == 4)
            def _():
                ag_copy(j, 1, st).wait_recv()
                fw_copy(j, 2, st).start()
                ag_copy(j, 2, st).wait_recv()
                fw_copy(j, 3, st).start()

    def run_events(j, lo, hi):
        def body(e, carry):
            service(j, e)
            return carry
        lax.fori_loop(lo, hi, body, 0)

    def norm_rows(j, l, st):
        rows = rows_of(st)
        ssq = jnp.zeros((R, BW), F32)
        for b in range(NB):
            xb = X[j, b, rows, :].astype(F32)
            ssq = ssq + xb * xb
        inv = lax.rsqrt(jnp.sum(ssq, axis=-1, keepdims=True) * (1.0 / D) + EPS)
        for b in range(NB):
            xb = X[j, b, rows, :].astype(F32)
            H[rows, b * BW:(b + 1) * BW] = (xb * inv * gain_v[l, :, b * BW:(b + 1) * BW]).astype(BF16)

    def norm(j, l):
        def body(st, carry):
            norm_rows(j, l, st)
            return carry
        lax.fori_loop(0, NS, body, 0)

    def drain(j, e0, l_next):
        run_events(j, e0, NE)

        def arrive(st, carry):
            for t in range(NY):
                fw_copy(j, t, st).wait_recv()

            @pl.when(l_next < L)
            def _():
                norm_rows(j, l_next, st)
            return carry
        lax.fori_loop(0, NS, arrive, 0)
        for bb in range(NY):
            pair_copy(j, bb).wait_send()

        def ends(st, carry):
            for t in range(NY - 1):
                rs_copy(j, t, st).wait_send()
                ag_copy(j, t, st).wait_send()
            for t in range(NY):
                fw_copy(j, t, st).wait_send()
            return carry
        lax.fori_loop(0, NS, ends, 0)

    def push_copy(j, l, d):
        g = 2 * xx + j
        return rcopy(KV.at[l, g], KV.at[l, g], s_kvs.at[j, d - 1], s_kvr.at[l * (2 * NX) + g], {'seq': lax.rem(s + 2 * d, 2 * NX)})

    def recv_wait(l, g):
        rcopy(KV.at[l, g], KV.at[l, g], s_kvs.at[0, 0], s_kvr.at[l * (2 * NX) + g], partner).wait_recv()

    def cache_local(l, j):
        return lcopy(KV.at[l, 2 * xx + j], kvout_h.at[l, c], s_cl.at[l])

    def cache_remote(l, j):
        return rcopy(KV.at[l, 2 * xx + j], kvout_h.at[l, c], s_cs.at[l], s_cr.at[l], partner)

    def qkv(j, l, slot):
        for n in range(NQ):
            QKVS[n] = jnp.dot(H[...], WQKV[:, n * 2 * HD:(n + 1) * 2 * HD], preferred_element_type=F32).astype(BF16)
        slot(0)
        g = 2 * xx + j

        def rot(val):
            vf = val.astype(F32)
            return (vf * TAB[j, 0] + pltpu.roll(vf, HD // 2, 1) * TAB[j, 1]).astype(BF16)
        KV[l, g, 0] = rot(QKVS[NQ - 1, :, 0:HD])
        KV[l, g, 1] = QKVS[NQ - 1, :, HD:2 * HD]
        for d in range(1, NX):
            @pl.when(xx + d < NX)
            def _():
                push_copy(j, l, d).start()

        @pl.when(c == j)
        def _():
            cache_local(l, j).start()

        @pl.when(c != j)
        def _():
            cache_remote(l, j).start()
        for h in range(GH):
            Q[j, h] = rot(QKVS[h // 2, :, (h % 2) * HD:(h % 2 + 1) * HD])

    def push_done(j, l):
        for d in range(1, NX):
            @pl.when(xx + d < NX)
            def _():
                push_copy(j, l, d).wait_send()

    def attention(j, l, slot):
        g = 2 * xx + j
        nt = (((1,), (1,)), ((), ()))
        QB = T // 2
        ex = scale * math.log2(math.e)

        row_i = lax.broadcasted_iota(jnp.int32, (QB, T), 0)
        col_i = lax.broadcasted_iota(jnp.int32, (QB, T), 1)

        def logits(h, qs, gi):
            return lax.dot_general(Q[j, h, qs], KV[l, gi, 0], nt, preferred_element_type=F32) * ex

        def rowmax(parts):
            top = parts[0]
            for part in parts[1:]:
                top = jnp.maximum(top, part)
            return jnp.max(top, axis=1, keepdims=True)

        def weigh(parts, m, gs):
            probs = [jnp.exp2(part - m) for part in parts]
            tot = probs[0]
            for part in probs[1:]:
                tot = tot + part
            out = jnp.dot(probs[0].astype(BF16), KV[l, gs[0], 1], preferred_element_type=F32)
            for part, gi in zip(probs[1:], gs[1:]):
                out = out + jnp.dot(part.astype(BF16), KV[l, gi, 1], preferred_element_type=F32)
            return jnp.sum(tot, axis=1, keepdims=True), out

        for h in range(GH):
            for q0 in range(0, T, QB):
                qs = slice(q0, q0 + QB)
                gs = [g - 1, g] if j == 1 else [g]
                parts = [logits(h, qs, gi) for gi in gs]
                parts[-1] = jnp.where(row_i + q0 >= col_i, parts[-1], -jnp.inf)
                m = rowmax(parts)
                tot, out = weigh(parts, m, gs)
                MX[h, qs] = jnp.broadcast_to(m, (QB, HD))
                LS[h, qs] = jnp.broadcast_to(tot, (QB, HD))
                ACC[h, qs] = out
        slot(0)

        def body(i, carry):
            gs = [2 * i, 2 * i + 1]
            if j == 0:
                for gi in gs:
                    recv_wait(l, gi)
            for h in range(GH):
                for q0 in range(0, T, QB):
                    qs = slice(q0, q0 + QB)
                    parts = [logits(h, qs, gi) for gi in gs]
                    m_old = MX[h, qs]
                    m_new = jnp.maximum(m_old, rowmax(parts))
                    tot, out = weigh(parts, jnp.concatenate([m_new] * (T // HD), axis=1), gs)
                    alpha = jnp.exp2(m_old - m_new)
                    MX[h, qs] = m_new
                    LS[h, qs] = LS[h, qs] * alpha + tot
                    ACC[h, qs] = ACC[h, qs] * alpha + out
            slot(i + 1)
            return carry
        lax.fori_loop(0, xx, body, 0)
        for h in range(GH):
            ATT[:, h * HD:(h + 1) * HD] = (ACC[h] / LS[h]).astype(BF16)

    def gate_up(j, l, n0, n1, slot):
        def act(n):
            gate = G[0]
            HID[:, pl.ds(pl.multiple_of(n * FT, FT), FT)] = (gate * jax.nn.sigmoid(gate) * G[1]).astype(BF16)

        def body(n, carry):
            i = (2 * l + j) * NGU + n
            sl = lax.rem(i, NGUBUF)
            for cp in gu_copies(i):
                cp.wait()
            act(jnp.maximum(n - 1, n0))
            for k in range(2):
                G[k] = jnp.dot(H[...], GU[sl, k], preferred_element_type=F32)

            @pl.when(n + NGUBUF < NGU)
            def _():
                for cp in gu_copies(i + NGUBUF):
                    cp.start()
            slot(n - n0)
            return carry
        lax.fori_loop(n0, n1, body, 0)
        act(n1 - 1)

    def o_tile(blk):
        cols = pl.ds(pl.multiple_of(blk * BW, BW), BW)
        return jnp.dot(ATT[...], WO[:, cols], preferred_element_type=F32)

    def send_pair(j, n):
        @pl.when(n < NY)
        def _():
            pair_copy(j, ring_block(n)).start()

    def down(j, l, with_o, slot):
        def body(m, carry):
            i = (2 * l + j) * NB + 2 * m
            for k in range(2):
                wd_copy(i + k).wait()
            for k in range(2):
                blk = block_of(2 * m + k)
                val = jnp.dot(HID[...], WD[lax.rem(i + k, NWDBUF)], preferred_element_type=F32)
                if with_o:
                    val = val + o_tile(blk)
                PS[j, blk] = val

            @pl.when(i + NWDBUF < 2 * L * NB)
            def _():
                for k in range(2):
                    wd_copy(i + NWDBUF + k).start()
            k0 = m - (NB // 2 - NGUBUF)

            @pl.when((k0 >= 0) & (2 * l + j + 1 < 2 * L))
            def _():
                for cp in gu_copies((2 * l + j + 1) * NGU + k0):
                    cp.start()
            if with_o:
                for k in range(2):
                    send_pair(j, 2 * m + k)
            slot(m)
            return carry
        lax.fori_loop(0, NB // 2, body, 0)

    def o_proj(j, l):
        def body(m, carry):
            for k in range(2):
                blk = block_of(2 * m + k)
                PS[j, blk] += o_tile(blk)
            for k in range(2):
                send_pair(j, 2 * m + k)
            return carry
        lax.fori_loop(0, NB // 2, body, 0)

    def layer(l, carry):
        def events(j, first):
            num, den = RATE[j]
            e_first = NS if (j == 1) else 0

            def slot(k):
                kk = first + k
                lo = jnp.minimum(e_first + lax.div(kk * num, den), NE)
                hi = jnp.minimum(e_first + lax.div((kk + 1) * num, den), NE)
                if j == 1:
                    hi = jnp.where(l > 0, hi, lo)
                run_events(j, lo, hi)
            return slot

        def reached(j, k):
            return jnp.minimum((NS if j == 1 else 0) + lax.div(k * RATE[j][0], RATE[j][1]), NE)

        qkv(0, l, events(1, 0))
        gate_up(0, l, 0, NGU, events(1, 1))
        down(0, l, False, events(1, 1 + NGU))

        @pl.when(l > 0)
        def _():
            drain(1, reached(1, jnp.int32(1 + NGU + NB // 2)), l)

        @pl.when(l == 0)
        def _():
            norm(1, l)

        qkv(1, l, lambda k: None)

        @pl.when(l + 1 < L)
        def _():
            for p in range(NRAW):
                raw_start(l + 1, jnp.int32(p))
        if NAHEAD:
            gate_up(1, l, 0, NAHEAD, lambda k: None)
        attention(0, l, lambda k: None)
        wo_copy(l).wait()
        o_proj(0, l)

        gate_up(1, l, NAHEAD, NGU, events(0, 0))
        k0 = NGU - NAHEAD
        attention(1, l, events(0, k0))
        k0 = k0 + xx + 1
        down(1, l, True, events(0, k0))
        e0 = reached(0, k0 + NB // 2)

        @pl.when(l + 1 < L)
        def _():
            wo_copy(l + 1).start()

            def one(k):
                lo = jnp.minimum(e0 + k, NE)
                run_events(0, lo, jnp.minimum(lo + 1, NE))
            build_qkv(l + 1, one)
        run_events(1, 0, NS)
        drain(0, jnp.minimum(jnp.where(l + 1 < L, e0 + NPQ + 2 * NPK, e0), NE), l + 1)
        push_done(0, l)
        push_done(1, l)
        return carry

    norm(0, 0)
    lax.fori_loop(0, L, layer, 0)
    drain(1, NS, L)

    for b in range(NB):
        lcopy(X.at[c, b], xout_h.at[:, pl.ds(b * BW, BW)], s_out.at[b]).start()
    for b in range(NB):
        lcopy(X.at[c, b], xout_h.at[:, pl.ds(b * BW, BW)], s_out.at[b]).wait()
    for l in range(L):
        cache_local(l, 0).wait()
        cache_remote(l, 0).wait()


def solution(mesh):
    NY = mesh.shape['head']
    NX = mesh.shape['seq'] // 2
    row_spec = P(('batch', 'seq'), None)
    pos_spec = P(('batch', 'seq'))
    head_spec = P(None, None, 'head', None)
    out_proj_spec = P(None, 'head', None, None)
    col_spec = P(None, None, 'head')
    down_spec = P(None, 'head', None)
    cache_spec = P(None, ('batch', 'seq'), 'head', None)

    def local_forward(x_loc, pos_loc, w_q, w_k, w_v, w_o, w_gate, w_up, w_down, norm_gain):
        T, D = x_loc.shape
        L, _, q_local, HD = w_q.shape
        GH = q_local // 2
        FF = w_gate.shape[2] // 2
        BW = D // (2 * NY)
        FT = 256 if FF % 256 == 0 else 128
        dims = dict(L=L, T=T, D=D, NY=NY, NX=NX, GH=GH, HD=HD, FF=FF, FT=FT, BW=BW)
        wq = w_q.reshape(L, D * q_local, HD)
        wk = w_k.reshape(L, D * 2, HD)
        wv = w_v.reshape(L, D * 2, HD)
        wo = w_o.reshape(L, q_local * HD, D)
        gain = norm_gain.astype(F32).reshape(L, 1, D)
        tab = rope_tables(pos_loc, HD)
        QW = GH * HD
        NB = 2 * NY
        NQ = (QW + 2 * HD) // (2 * HD)
        RP = min(2048, D * 2)
        any_spec = pl.BlockSpec(memory_space=pl.ANY)
        dma = pltpu.SemaphoreType.DMA
        V = pltpu.VMEM
        scratch = [
            V((2, NB, T, BW), BF16), V((T, D), BF16), V((NQ, T, 2 * HD), BF16), V((2, GH, T, HD), BF16), V((T, QW), BF16),
            V((T, FF), BF16), V((2, T, FT), F32), V((2, NB, T, BW), F32), V((2, NY, T, BW), F32), V((2, NY - 1, T, BW), F32),
            V((2, 2, T, HD), F32), V((L, 2 * NX, 2, T, HD), BF16), V((NGUBUF, 2, D, FT), BF16), V((NWDBUF, FF, BW), BF16),
            V((QW, D), BF16), V((D, QW + 2 * HD), BF16), V((GH, T, HD), F32), V((GH, T, HD), F32), V((GH, T, HD), F32),
            V((NRAW, RP, HD), BF16), V((RP, HD), F32),
            dma((NB,)), dma((NB,)), dma((NB,)), dma((3,)), dma((NGUBUF, 2)), dma((NWDBUF,)), dma((1,)), dma((NRAW,)),
            dma((2, NY)), dma((2, NY)), dma((2, NY - 1, NSTREAM)), dma((2, NY - 1, NSTREAM)),
            dma((2, NY - 1, NSTREAM)), dma((2, NY - 1, NSTREAM)), dma((2, NY, NSTREAM)), dma((2, NY, NSTREAM)),
            dma((2, NX)), dma((L * 2 * NX,)), dma((L,)), dma((L,)), dma((L,)), dma((NB,)),
        ]
        x_out, kv = pl.pallas_call(
            functools.partial(decoder_kernel, dims),
            out_shape=(jax.ShapeDtypeStruct((T, D), BF16), jax.ShapeDtypeStruct((L, 2, 2, T, HD), BF16)),
            in_specs=[any_spec] * 9 + [pl.BlockSpec(memory_space=pltpu.VMEM)],
            out_specs=(any_spec, any_spec),
            scratch_shapes=scratch,
            compiler_params=pltpu.CompilerParams(collective_id=0, has_side_effects=True, vmem_limit_bytes=67043328),
            name='decoder',
        )(x_loc, tab, wq, wk, wv, wo, w_gate, w_up, w_down, gain)
        kv = jnp.transpose(kv, (2, 0, 3, 1, 4))
        return x_out, kv[0], kv[1]

    return jax.shard_map(local_forward, mesh=mesh, in_specs=(row_spec, pos_spec, head_spec, head_spec, head_spec, out_proj_spec, col_spec, col_spec, down_spec, P(None, None)), out_specs=(row_spec, cache_spec, cache_spec), check_vma=False)
```
